256 devices in a mesh: dp: 64 (over y_hi, z, x), mp: 4 (over y_lo, core).
Axes of the slice: x: 4, y: 4 (y_hi: 2, y_lo: 2; y = y_hi * 2 + y_lo), z: 8, core: 2. Of those that a mesh axis runs over, the one named last changes fastest.
Arguments:
- observations: bfloat16 [212992, 2048], P('dp', 'mp'), may hold values from -140 to 140
- layer_weights: bfloat16 [2, 2048, 2048], P(None, 'dp', 'mp'), may hold values from -0.1875 to 0.1875
- head_weights: bfloat16 [2048, 18], P('mp'), may hold values from -0.1875 to 0.1875
- rewards: float32 [3328, 64], P('dp'), may hold values from -6 to 6
- actions: int32 [3328, 64], P('dp'), may hold values from 0 to 17
- done_flags: int32 [3328, 64], P('dp'), may hold values 0 or 1
- behaviour: float32 [3328, 64], P('dp'), may hold values from 0.05 to 1
Outputs:
- targets: float32 [3328, 64], P('dp')
The draws below stay inside these ranges and needn't reach their ends.
All inputs are finite; a program needn't handle non-finite values. No bound on the sum of `done_flags` on one device may be relied on, other than what follows from the above.
Results may differ from the reference program's by a relative error of at most 0.0056.
Values may be sent and summed in bfloat16 or wider, within the bound.
A program may use at most 128 MiB of HBM per device.

```python
import math
import jax
import jax.numpy as jnp
from jax import lax

W = 2048
A = 18
LAYERS = 2
LEN = 64
SEQS = 3328
ROWS = 212992


def draw_observations(key, part):
    first, second = jax.random.split(jax.random.fold_in(key, 11), 2)
    scales = jnp.exp(jax.random.uniform(second, (ROWS, 1), jnp.float32) * jnp.log(10.0))
    values = jnp.clip(jax.random.normal(first, (ROWS, W), jnp.float32), -4.0, 4.0) * scales
    return values.astype(jnp.bfloat16)


def touch_ends(result, own_key, smallest, high):
    longest = result.shape.index(max(result.shape))
    spots = []
    for shift in (0, 1):
        where = [jax.random.randint(jax.random.fold_in(own_key, axis), (), 0, length) for axis, length in enumerate(result.shape)]
        where[longest] = (where[longest] + shift) % result.shape[longest]
        spots.append(tuple(where))
    return result.at[spots[0]].set(smallest).at[spots[1]].set(high)


def levels(own_key, shape, pieces, smallest, high):
    gain = 1.0
    for position, parts in pieces:
        heights = jax.random.uniform(jax.random.fold_in(jax.random.fold_in(own_key, 6), position), (parts,), jnp.float32, smallest / len(pieces), high / len(pieces))
        gain = gain * jnp.repeat(jnp.exp(heights), shape[position] // parts).reshape((-1,) + (1,) * (len(shape) - 1 - position))
    return gain


def noise(stream_key, dims, scale, bound, cuts=(), kind=jnp.bfloat16):
    gain = levels(stream_key, dims, cuts, -0.22, 0.18) if cuts else 1.0
    result = jax.random.normal(stream_key, dims, jnp.float32) * scale * gain
    return jnp.minimum(jnp.maximum(result, -bound), bound).astype(kind)


def setup_inputs(seed: int = 0) -> dict:
    streams_of = jax.random.split(jax.random.key(seed), 8)
    observations = draw_observations(jax.random.fold_in(streams_of[7], 71), 0)
    layer_weights = noise(streams_of[1], (LAYERS, W, W), (W // 2) ** -0.5, 0.1875, ((1, 64), (2, 4)))
    head_weights = noise(streams_of[2], (W, A), (W // 2) ** -0.5, 0.1875, ((0, 4),))
    rewards = noise(streams_of[3], (SEQS, LEN), 1.0, 6.0, ((0, 64),), jnp.float32)
    actions = touch_ends(jax.random.randint(streams_of[4], (SEQS, LEN), 0, A), jax.random.fold_in(streams_of[4], 1), 0, A - 1).astype(jnp.int32)
    done_flags = touch_ends((jax.random.randint(streams_of[5], (SEQS, LEN), 0, 16) < 1).astype(jnp.int32), jax.random.fold_in(streams_of[5], 1), 0, 1)
    behaviour = jnp.clip(jnp.exp(math.log(1.0) - 2.9957323 * jax.random.uniform(streams_of[6], (SEQS, LEN), jnp.float32) ** levels(streams_of[6], (SEQS, LEN), ((0, 64),), -0.2, 0.2)), 0.05, 1.0)
    return dict(observations=observations, layer_weights=layer_weights, head_weights=head_weights, rewards=rewards, actions=actions, done_flags=done_flags, behaviour=behaviour)


def retrace(qvals, rewards, actions, done_flags, behaviour):
    seqs = rewards.shape[0]
    length = rewards.shape[1]
    qvals = qvals.reshape(seqs, length, A)
    probs = jax.nn.softmax(4.0 * qvals, axis=-1)
    value = jnp.sum(probs * qvals, axis=-1)
    onehot = (actions[:, :, None] == jnp.arange(A, dtype=jnp.int32)[None, None, :]).astype(qvals.dtype)
    taken = jnp.sum(onehot * qvals, axis=-1)
    chosen = jnp.sum(onehot * probs, axis=-1)
    trace = 0.95 * jnp.minimum(1.0, chosen / behaviour)
    keep = 0.99 * (1.0 - done_flags.astype(qvals.dtype))

    def stepper(later, inputs):
        reward_t, keep_t, value_n, trace_n, taken_n = inputs
        now = reward_t + keep_t * (value_n + trace_n * (later - taken_n))
        return now, now

    inputs = (rewards[:, :-1].T, keep[:, :-1].T, value[:, 1:].T, trace[:, 1:].T, taken[:, 1:].T)
    last = taken[:, length - 1]
    final, earlier = lax.scan(stepper, last, inputs, reverse=True)
    return jnp.concatenate([earlier.T, last[:, None]], axis=1)


def reference(observations, layer_weights, head_weights, rewards, actions, done_flags, behaviour):
    hidden = observations
    for layer in range(LAYERS):
        hidden = jax.nn.relu(jnp.dot(hidden, layer_weights[layer], preferred_element_type=jnp.float32)).astype(jnp.bfloat16)
    qvals = jnp.dot(hidden, head_weights, preferred_element_type=jnp.float32)
    return retrace(qvals, rewards, actions, done_flags, behaviour)
```

```python
import jax
import jax.numpy as jnp
from jax import lax
from jax.experimental import pallas as pl
from jax.experimental.pallas import tpu as pltpu
from jax.sharding import Mesh
from jax.sharding import PartitionSpec as P

MESH = pl.DeviceIdType.MESH
AXES = ("yh", "z", "x", "yl", "core")
DP = ("yh", "z", "x")
MP = ("yl", "core")
NX, NZ = 4, 8
CHUNKS = 4
GAP = 2

SLOTS = (
    ((0, 0, 0), (1, 0, 0), (2, 0, 0), (3, 0, 0), (4, 0, 0)),
    ((0, 1, 0), (1, 1, 0), (2, 1, 0), (3, 1, 0), (4, 1, 0)),
    ((0, 0, 24), (1, 0, 7), (2, 0, 7), (3, 0, 32), (4, 0, 7)),
    ((0, 0, 8), (1, 0, 8), (2, 0, 1), (3, 0, 8), (4, 0, 32)),
    ((0, 0, 6), (1, 0, 15), (2, 0, 33), (3, 0, 1), (4, 0, 56)),
    ((0, 0, 15), (1, 0, 6), (2, 0, 25), (3, 0, 33), (4, 0, 6)),
    ((0, 0, 23), (1, 0, 38), (2, 0, 57), (3, 0, 57), (4, 0, 23)),
    ((0, 0, 5), (1, 0, 33), (2, 0, 38), (3, 0, 34), (4, 0, 5)),
    ((0, 0, 16), (1, 0, 34), (2, 0, 58), (3, 0, 58), (4, 0, 55)),
    ((0, 0, 62), (1, 0, 37), (2, 0, 4), (3, 0, 35), (4, 0, 62)),
    ((0, 0, 42), (1, 0, 5), (2, 0, 59), (3, 0, 59), (4, 0, 22)),
    ((0, 0, 61), (1, 0, 4), (2, 0, 61), (3, 0, 42), (4, 0, 45)),
    ((0, 0, 51), (1, 0, 10), (2, 0, 2), (3, 0, 51), (4, 0, 21)),
    ((0, 0, 35), (1, 1, 32), (2, 1, 1), (3, 0, 10), (4, 0, 28)),
    ((0, 1, 1), (1, 1, 7), (2, 1, 24), (3, 1, 1), (4, 1, 7)),
    ((0, 1, 25), (1, 1, 40), (2, 1, 25), (3, 1, 25), (4, 1, 40)),
    ((0, 1, 2), (1, 1, 2), (2, 1, 6), (3, 1, 40), (4, 1, 6)),
    ((0, 1, 26), (1, 1, 47), (2, 1, 26), (3, 1, 48), (4, 1, 47)),
    ((0, 1, 30), (1, 1, 34), (2, 1, 30), (3, 1, 26), (4, 1, 30)),
    ((0, 1, 5), (1, 1, 5), (2, 1, 58), (3, 1, 58), (4, 1, 55)),
    ((0, 1, 29), (1, 1, 15), (2, 1, 27), (3, 1, 42), (4, 1, 22)),
    ((0, 1, 13), (1, 1, 6), (2, 1, 59), (3, 1, 59), (4, 1, 54)),
    ((0, 1, 6), (1, 1, 1), (2, 1, 7), (3, 1, 43), (4, 1, 13)),
    ((0, 1, 7), (1, 1, 60), (2, 1, 32), (3, 1, 51), (4, 1, 21)),
    ((0, 1, 31), (1, 1, 59), (2, 1, 12), (3, 1, 10), (4, 1, 29)),
    ((3, 1, 2),),
)
STEPS = ((1, 0, 0), (0, 1, 0), (0, 3, 0), (0, 0, 1), (0, 0, 7))


def split(code):
    return code // 32, code // 8 % 4, code % 8


def moved(code, link):
    pair, dx, dz = split(code)
    a, b, c = STEPS[link]
    return ((pair + a) % 2 * 4 + (dx + b) % 4) * 8 + (dz + c) % 8


def kernel(
    obs, own_w, own_head, rewards, actions, done, behaviour, out,
    wg, xb, h1, heads, lanes, cols, tsend, trecv,
    w_recv, i_recv, d_recv, i_send, r_send, d_send,
    o_recv, o_send, o_local, h_recv, h_send, t_recv, t_send,
):
    yh, z, x = lax.axis_index("yh"), lax.axis_index("z"), lax.axis_index("x")
    yl, core = lax.axis_index("yl"), lax.axis_index("core")
    rows_all, width = xb.shape
    depth, part = own_w.shape[1], own_w.shape[2]
    seqs, length = rows_all // rewards.shape[1], rewards.shape[1]
    step_rows = rows_all // CHUNKS
    acts = own_head.shape[0]
    packets = 2 * NX * NZ

    xp, xm = lax.rem(x + 1, NX), lax.rem(x + NX - 1, NX)
    zp, zm = lax.rem(z + 1, NZ), lax.rem(z + NZ - 1, NZ)
    links = (
        {"yh": 1 - yh, "yl": 1 - yl},
        {"x": xp},
        {"x": xm},
        {"z": zp},
        {"z": zm},
    )
    peers = (None, {"core": 1 - core}, {"yl": 1 - yl}, {"yl": 1 - yl, "core": 1 - core})
    mine = yl * 2 + core
    peer_mp = (
        mine,
        yl * 2 + (1 - core),
        (1 - yl) * 2 + core,
        (1 - yl) * 2 + (1 - core),
    )

    y_from = (yh, 1 - yh)
    x_from = tuple(lax.rem(x + NX - k, NX) for k in range(NX))
    z_from = tuple(lax.rem(z + NZ - k, NZ) for k in range(NZ))

    def rows_of(code):
        a, b, c = split(code)
        start = ((y_from[a] * NZ + z_from[c]) * NX + x_from[b]) * depth
        return pl.ds(pl.multiple_of(start, depth), depth)

    own_rows = rows_of(0)

    def whole(layer, code, side):
        return wg.at[layer, side, :, rows_of(code), :]

    def half(layer, which):
        return wg.at[layer, core, which, own_rows, :]

    barrier = pltpu.get_barrier_semaphore()
    for target in links + peers[1:]:
        pl.semaphore_signal(barrier, inc=1, device_id=target, device_id_type=MESH)
    pl.semaphore_wait(barrier, len(links) + 3)

    def remote(src, dst, send, recv, target):
        return pltpu.make_async_remote_copy(
            src_ref=src, dst_ref=dst, send_sem=send, recv_sem=recv,
            device_id=target, device_id_type=MESH,
        )

    def forward(layer, ref):
        remote(ref, ref, d_send.at[layer], d_recv.at[layer], peers[1]).start()

    for layer in range(2):
        remote(own_w.at[layer], half(layer, yl), i_send.at[layer], i_recv.at[layer], peers[2]).start()
    for slot in SLOTS[:2]:
        for link, layer, code in slot:
            assert code == 0
            remote(
                own_w.at[layer], half(layer, yl), r_send.at[layer],
                w_recv.at[layer, moved(0, link)], links[link],
            ).start()
    for m in range(1, 4):
        remote(own_head, heads.at[mine], h_send.at[m], h_recv.at[m], peers[m]).start()
    for layer in range(2):
        remote(
            own_w.at[layer], half(layer, yl), d_send.at[layer], d_recv.at[layer], peers[1]
        ).start()

    my_cols = pl.ds(pl.multiple_of(mine * part, part), part)

    def chunk_of(m, k):
        start = peer_mp[m] * rows_all + k * step_rows
        return obs.at[pl.ds(pl.multiple_of(start, step_rows), step_rows), :]

    for k in range(CHUNKS):
        here = pl.ds(k * step_rows, step_rows)
        pltpu.make_async_copy(chunk_of(0, k), xb.at[here, my_cols], o_local.at[k]).start()
        for m in (2, 3, 1):
            remote(
                chunk_of(m, k), xb.at[here, my_cols], o_send.at[m], o_recv.at[m, k], peers[m]
            ).start()

    for layer in range(2):
        wg[layer, core, yl, own_rows, :] = own_w[layer]
    heads[mine] = own_head[...]

    first = mine * seqs
    for s in range(seqs):
        lanes[0:1, s * length : (s + 1) * length] = actions[pl.ds(first + s, 1), :]
        cols[3, s : s + 1, :length] = behaviour[pl.ds(first + s, 1), :]
        cols[4, s : s + 1, :length] = rewards[pl.ds(first + s, 1), :]
        cols[5, s : s + 1, :length] = 0.99 * (
            1.0 - done[pl.ds(first + s, 1), :].astype(jnp.float32)
        )

    for layer in range(2):
        ref = half(layer, 1 - yl)
        remote(ref, ref, i_send.at[layer], i_recv.at[layer], peers[2]).wait_recv()
        for link, at, code in SLOTS[layer]:
            assert at == layer
            remote(
                ref, ref, r_send.at[layer], w_recv.at[layer, moved(0, link)], links[link]
            ).start()
        forward(layer, ref)

    def arrive(slot):
        for link, layer, code in slot:
            got = moved(code, link)
            ref = whole(layer, got, core)
            remote(ref, ref, r_send.at[layer], w_recv.at[layer, got], links[link]).wait_recv()
            forward(layer, ref)

    def send(slot):
        for link, layer, code in slot:
            ref = whole(layer, code, core)
            remote(
                ref, ref, r_send.at[layer], w_recv.at[layer, moved(code, link)], links[link]
            ).start()

    def partner_done(layer):
        ref = wg.at[layer, 1 - core]
        remote(ref, ref, d_send.at[layer], d_recv.at[layer], peers[1]).wait_recv()

    def chunk_done(k):
        here = pl.ds(k * step_rows, step_rows)
        dst = xb.at[here, my_cols]
        pltpu.make_async_copy(chunk_of(0, k), dst, o_local.at[k]).wait()
        for m in (1, 2, 3):
            dst = xb.at[here, pl.ds(pl.multiple_of(peer_mp[m] * part, part), part)]
            remote(dst, dst, o_send.at[m], o_recv.at[m, k], peers[m]).wait_recv()

    def first_layer(k):
        here = pl.ds(k * step_rows, step_rows)

        def column(j, carry):
            c, y = j // 2, j % 2
            total = jnp.dot(xb[here, :], wg[0, c, y], preferred_element_type=jnp.float32)
            place = pl.ds(pl.multiple_of((y * 2 + c) * part, part), part)
            h1[here, place] = jnp.maximum(total, 0.0).astype(jnp.bfloat16)
            return carry

        lax.fori_loop(0, 4, column, 0)

    last0 = max(t for t, slot in enumerate(SLOTS) if any(at == 0 for _, at, _ in slot))
    end = len(SLOTS)
    compute_at = {last0 + GAP + 1 + n * 3: n for n in range(CHUNKS)}
    todo = 0
    for t in range(2, end + GAP):
        if t >= GAP:
            arrive(SLOTS[t - GAP])
        if t < end:
            send(SLOTS[t])
        if t in compute_at:
            k = compute_at[t]
            if k == 0:
                partner_done(0)
            chunk_done(k)
            first_layer(k)
            todo = k + 1
    for k in range(todo, CHUNKS):
        chunk_done(k)
        first_layer(k)
    partner_done(1)

    def second_layer(i, carry):
        here = pl.ds(pl.multiple_of(i * step_rows, step_rows), step_rows)
        for c in range(2):
            for y in range(2):
                total = jnp.dot(h1[here, :], wg[1, c, y], preferred_element_type=jnp.float32)
                place = pl.ds((y * 2 + c) * part, part)
                xb[here, place] = jnp.maximum(total, 0.0).astype(jnp.bfloat16)
        return carry

    lax.fori_loop(0, CHUNKS, second_layer, 0)

    for m in range(1, 4):
        dst = heads.at[peer_mp[m]]
        remote(dst, dst, h_send.at[m], h_recv.at[m], peers[m]).wait_recv()
    q = jnp.zeros((acts, rows_all), jnp.float32)
    for m in range(4):
        q += lax.dot_general(
            heads[m], xb[:, m * part : (m + 1) * part], (((1,), (1,)), ((), ())),
            preferred_element_type=jnp.float32,
        )

    peak = jnp.max(q, axis=0, keepdims=True)
    powers = jnp.exp(4.0 * (q - peak))
    probs = powers / jnp.sum(powers, axis=0, keepdims=True)
    value = jnp.sum(probs * q, axis=0, keepdims=True)
    picked = lax.broadcasted_iota(jnp.int32, (acts, rows_all), 0) == lanes[0:1, :rows_all]
    taken = jnp.sum(jnp.where(picked, q, 0.0), axis=0, keepdims=True)
    chosen = jnp.sum(jnp.where(picked, probs, 0.0), axis=0, keepdims=True)
    for s in range(seqs):
        at = slice(s * length, (s + 1) * length)
        cols[0, s : s + 1, :length] = value[:, at]
        cols[1, s : s + 1, :length] = taken[:, at]
        cols[2, s : s + 1, :length] = chosen[:, at]

    taken = cols[1]
    trace = 0.95 * jnp.minimum(1.0, cols[2] / cols[3])
    step = lax.broadcasted_iota(jnp.int32, taken.shape, 1)

    def later(a, k):
        return pltpu.roll(a, taken.shape[1] - k, 1)

    keep = cols[5]
    inner = step < length - 1
    slope = jnp.where(inner, keep * later(trace, 1), 0.0)
    base = jnp.where(
        inner,
        cols[4] + keep * (later(cols[0], 1) - later(trace * taken, 1)),
        taken,
    )
    base = jnp.where(step < length, base, 0.0)
    k = 1
    while k < length:
        base = base + slope * later(base, k)
        slope = slope * later(slope, k)
        k *= 2

    tsend[...] = base
    trecv[mine] = base
    for m in (2, 3, 1):
        remote(tsend, trecv.at[mine], t_send.at[m], t_recv.at[m], peers[m]).start()

    for layer in range(2):
        remote(own_w.at[layer], half(layer, yl), i_send.at[layer], i_recv.at[layer], peers[2]).wait_send()
        ref = wg.at[layer, 0, :, pl.ds(0, (packets - 1) * depth), :]
        remote(ref, ref, r_send.at[layer], d_recv.at[layer], peers[1]).wait_send()
        ref = wg.at[layer, 0]
        remote(ref, ref, d_send.at[layer], d_recv.at[layer], peers[1]).wait_send()
    for m in range(1, 4):
        dst = xb.at[:, my_cols]
        src = obs.at[pl.ds(0, rows_all), :]
        remote(src, dst, o_send.at[m], o_recv.at[m, 0], peers[m]).wait_send()
        remote(own_head, heads.at[mine], h_send.at[m], h_recv.at[m], peers[m]).wait_send()
    for m in (1, 2, 3):
        dst = trecv.at[peer_mp[m]]
        remote(tsend, dst, t_send.at[m], t_recv.at[m], peers[m]).wait()
    for m in range(4):
        out[m * seqs : (m + 1) * seqs, :] = trecv[m, :seqs, :length]


def per_device(obs, layers, head, rewards, actions, done, behaviour):
    depth, part = layers.shape[1], layers.shape[2]
    rows_all, width = obs.shape[0] // 4, part * 4
    acts = head.shape[1]
    dma = pltpu.SemaphoreType.DMA
    vmem = pl.BlockSpec(memory_space=pltpu.VMEM)
    lanes = -(-rows_all // 128) * 128
    return pl.pallas_call(
        kernel,
        out_shape=jax.ShapeDtypeStruct(rewards.shape, jnp.float32),
        in_specs=[pl.BlockSpec(memory_space=pl.ANY)] + [vmem] * 6,
        out_specs=vmem,
        scratch_shapes=[
            pltpu.VMEM((2, 2, 2, width, part), jnp.bfloat16),
            pltpu.VMEM((rows_all, width), jnp.bfloat16),
            pltpu.VMEM((rows_all, width), jnp.bfloat16),
            pltpu.VMEM((4, acts, part), jnp.bfloat16),
            pltpu.VMEM((8, lanes), jnp.int32),
            pltpu.VMEM((6, 16, 128), jnp.float32),
            pltpu.VMEM((16, 128), jnp.float32),
            pltpu.VMEM((4, 16, 128), jnp.float32),
            dma((2, 2 * NX * NZ)),
            dma((2,)), dma((2,)), dma((2,)), dma((2,)), dma((2,)),
            dma((4, CHUNKS)), dma((4,)), dma((CHUNKS,)),
            dma((4,)), dma((4,)), dma((4,)), dma((4,)),
        ],
        compiler_params=pltpu.CompilerParams(
            collective_id=0, has_side_effects=True, vmem_limit_bytes=60 * 2**20
        ),
    )(obs, layers, head.T, rewards, actions, done, behaviour)


def solution(mesh):
    devices = mesh.devices.reshape(2, NZ, NX, 2, 2)
    laid = Mesh(devices, AXES)
    placed = (
        P(DP, MP),
        P(None, DP, MP),
        P(MP, None),
        P(DP, None),
        P(DP, None),
        P(DP, None),
        P(DP, None),
    )
    return jax.shard_map(
        per_device, mesh=laid, in_specs=placed, out_specs=P(DP, None), check_vma=False
    )
```
